32 devices in a mesh: pts: 16 (over z, x, core), tau: 2 (over y).
Axes of the slice: x: 2, y: 2, z: 4, core: 2. Of those that a mesh axis runs over, the one named last changes fastest.
Arguments:
- occupied_values: float32 [256, 512], P(('pts', 'tau')), may hold values from -2.5 to 2.5
- virtual_values: float32 [256, 1536], P(('pts', 'tau')), may hold values from -1.75 to 1.75
- occupied_energy: float32 [512], replicated, may hold values from -1 to -0.05
- virtual_energy: float32 [1536], replicated, may hold values from 0.05 to 2
- tau_points: float32 [2], replicated, may hold values from 0.1 to 3
- tau_weights: float32 [2], replicated, may hold values from 0.2 to 1
- frequencies: float32 [2], replicated, may hold values from 0.1 to 3
- pair_live: int32 [16, 16], P('pts'), may hold values from 0 to 1, as said below
Outputs:
- polarizability: float32 [2, 256, 2, 128], P(None, 'pts', 'tau')
The draws below stay inside these ranges and needn't reach their ends.
Inputs may be any that keep to these rules, and one draw needn't show every extreme that they name: `pair_live`: 1 marks a block pair that is formed, 0 one that is left out; every diagonal entry is 1.
All inputs are finite; a program needn't handle non-finite values.
Results may differ from the reference program's by a relative error of at most 0.000076.
Values sent between devices are 32-bit elements; how exact they have to be, the bound alone decides.
No kernel may reach another device: no remote copies, remote signals or barrier semaphores. Data moves between devices by JAX's collectives and lax.ppermute only.
A program may use at most 64 MiB of HBM per device.

```python
import math
import jax
import jax.numpy as jnp
from jax import lax

PTS_DEV = 8
NOCC = 512
NEMP = 1536
NBLK = 16
POINTS = 256
NTAU = 2
NFREQ = 2


def draw_pair_live(key, part):
    base = jax.random.fold_in(key, 11)
    key_rate, key_cell = jax.random.split(base)
    density = jax.random.randint(key_rate, (NBLK, 1), 1, 7)
    cells = jax.random.randint(key_cell, (NBLK, NBLK), 0, 6)
    diagonal = jnp.arange(NBLK)[:, None] == jnp.arange(NBLK)[None, :]
    return jnp.where((cells < density) | diagonal, 1, 0).astype(jnp.int32)


def steps_of(key, extent, shards, least, top_value):
    loudness = 1.0
    for position, parts in shards:
        steps = jax.random.uniform(jax.random.fold_in(jax.random.fold_in(key, 6), position), (parts,), jnp.float32, least / len(shards), top_value / len(shards))
        loudness = loudness * jnp.repeat(jnp.exp(steps), extent[position] // parts).reshape((-1,) + (1,) * (len(extent) - 1 - position))
    return loudness


def noise(rng, dims, spread, bound, shards=(), dtype=jnp.bfloat16):
    loudness = steps_of(rng, dims, shards, -0.22, 0.18) if shards else 1.0
    drawn = jax.random.normal(rng, dims, jnp.float32) * spread * loudness
    return jnp.minimum(jnp.maximum(drawn, -bound), bound).astype(dtype)


def setup_inputs(seed: int = 0) -> dict:
    keys = jax.random.split(jax.random.key(seed), 9)
    occupied_values = noise(keys[0], (POINTS, NOCC), 0.18, 2.5, ((0, 32),), jnp.float32)
    virtual_values = noise(keys[1], (POINTS, NEMP), 0.11, 1.75, ((0, 32),), jnp.float32)
    occupied_energy = jnp.clip(jax.random.uniform(keys[2], (NOCC,), jnp.float32, -1.0, -0.05), -1.0, -0.05)
    virtual_energy = jnp.clip(jax.random.uniform(keys[3], (NEMP,), jnp.float32, 0.05, 2.0), 0.05, 2.0)
    tau_points = jnp.clip(jnp.exp(jax.random.uniform(keys[4], (NTAU,), jnp.float32, math.log(0.1), math.log(3.0))), 0.1, 3.0)
    tau_weights = jnp.clip(jnp.exp(jax.random.uniform(keys[5], (NTAU,), jnp.float32, math.log(0.2), math.log(1.0))), 0.2, 1.0)
    frequencies = jnp.clip(jnp.exp(jax.random.uniform(keys[6], (NFREQ,), jnp.float32, math.log(0.1), math.log(3.0))), 0.1, 3.0)
    pair_live = draw_pair_live(jax.random.fold_in(keys[8], 71), 0)
    return {"occupied_values": occupied_values, "virtual_values": virtual_values, "occupied_energy": occupied_energy, "virtual_energy": virtual_energy, "tau_points": tau_points, "tau_weights": tau_weights, "frequencies": frequencies, "pair_live": pair_live}


def reference(occupied_values, virtual_values, occupied_energy, virtual_energy, tau_points, tau_weights, frequencies, pair_live):
    highest = lax.Precision.HIGHEST
    block_pts = POINTS // NBLK
    live_mask = jnp.repeat(jnp.repeat(pair_live, block_pts, axis=0), block_pts, axis=1).astype(jnp.float32)

    def one_time(moment):
        occupied_scaled = occupied_values * jnp.exp(occupied_energy * moment)[None, :]
        virtual_scaled = virtual_values * jnp.exp(-virtual_energy * moment)[None, :]
        green_occupied = jnp.dot(occupied_scaled, occupied_values.T, precision=highest, preferred_element_type=jnp.float32)
        green_virtual = jnp.dot(virtual_scaled, virtual_values.T, precision=highest, preferred_element_type=jnp.float32)
        return -(green_occupied * green_virtual) * live_mask

    chi_time = lax.map(one_time, tau_points)
    mixing = 2.0 * tau_weights[None, :] * jnp.cos(frequencies[:, None] * tau_points[None, :])
    chi_freq = jnp.einsum("kt,tpq->kpq", mixing, chi_time, precision=highest)
    grouped = chi_freq.reshape(NFREQ, POINTS, NBLK, NTAU, PTS_DEV)
    grouped = jnp.transpose(grouped, (0, 1, 3, 2, 4))
    return grouped.reshape(NFREQ, POINTS, NTAU, NBLK * PTS_DEV)
```

```python
import functools

import jax
import jax.numpy as jnp
from jax import lax
from jax.sharding import PartitionSpec as P

AXES = ("pts", "tau")
DIRECT = 4


def layout(mesh):
    points, groups = mesh.shape["pts"], mesh.shape["tau"]
    cores = 2 if points % 2 == 0 else 1
    pairs = 2 if points % (2 * cores) == 0 else 1
    return points // (pairs * cores), pairs, cores, groups


def gather(mesh, dim, block):
    sizes = layout(mesh)
    strides = (sizes[1] * sizes[2] * sizes[3], sizes[2] * sizes[3], sizes[3], 1)
    size, stride, n = sizes[dim], strides[dim], sizes[0] * strides[0]
    mine = (lax.axis_index(AXES) // stride) % size
    if size <= DIRECT and size & (size - 1) == 0:
        blocks, coords = [block], [mine]
        for step in range(size - 1, 0, -1):
            pairs = [(i, i + (((i // stride) % size) ^ step) * stride - ((i // stride) % size) * stride) for i in range(n)]
            blocks.append(lax.ppermute(block, AXES, pairs))
            coords.append(mine ^ step)
        return blocks, coords
    firsts = [i for i in range(n) if (i // stride) % size == 0]
    members = [[i + k * stride for k in range(size)] for i in firsts]
    every = lax.all_gather(block, AXES, axis=0, axis_index_groups=members)
    order = [(mine + k) % size for k in range(size)]
    return [every[k] for k in order], order


def on_device(
    mesh,
    occupied_values,
    virtual_values,
    occupied_energy,
    virtual_energy,
    tau_points,
    tau_weights,
    frequencies,
    pair_live,
):
    highest = lax.Precision.HIGHEST
    device_pts, n_occupied = occupied_values.shape
    far, pairs, cores, groups = layout(mesh)
    me = lax.axis_index("pts")
    pair = (me // cores) % pairs

    own = jnp.concatenate([occupied_values, virtual_values], axis=1)
    far_blocks, far_at = gather(mesh, 0, own)
    row_blocks, row_at = gather(mesh, 3, own)
    rows = jnp.concatenate(row_blocks, axis=0)
    row_sets, _ = gather(mesh, 1, rows)
    column_sets, core_at = gather(mesh, 2, jnp.concatenate(far_blocks, axis=0))
    columns = jnp.concatenate(column_sets, axis=0)

    occupied_decay = jnp.exp(occupied_energy[None, :] * tau_points[:, None])[:, None, :]
    virtual_decay = jnp.exp(-virtual_energy[None, :] * tau_points[:, None])[:, None, :]
    mixing = 2.0 * tau_weights[None, :] * jnp.cos(frequencies[:, None] * tau_points[None, :])

    def chi_of(part):
        green_occupied = jnp.einsum(
            "trw,nw->trn", part[None, :, :n_occupied] * occupied_decay, columns[:, :n_occupied], precision=highest
        )
        green_virtual = jnp.einsum(
            "trw,nw->trn", part[None, :, n_occupied:] * virtual_decay, columns[:, n_occupied:], precision=highest
        )
        return jnp.einsum("kt,trn->krn", mixing, -(green_occupied * green_virtual), precision=highest)

    n = far * pairs * cores * groups
    results, result_at = [chi_of(rows)], [pair]
    for step in range(1, pairs):
        swap = cores * groups * step
        there = chi_of(row_sets[step])
        results.append(lax.ppermute(there, AXES, [(i, i ^ swap) for i in range(n)]))
        result_at.append(pair ^ step)

    blocks = jnp.stack(
        [(f * pairs + x) * cores + c for x in result_at for c in core_at for f in far_at]
    )
    place = (blocks[:, None] * device_pts + jnp.arange(device_pts)[None, :]).reshape(-1)
    spread = (place[:, None] == jnp.arange(place.shape[0])[None, :]).astype(jnp.float32)
    chi = jnp.einsum("krm,mn->krn", jnp.concatenate(results, axis=-1), spread, precision=highest)
    row_place = (jnp.stack(row_at)[:, None] * device_pts + jnp.arange(device_pts)[None, :]).reshape(-1)
    row_spread = (row_place[None, :] == jnp.arange(row_place.shape[0])[:, None]).astype(jnp.float32)
    chi = jnp.einsum("sr,krn->ksn", row_spread, chi, precision=highest)
    column_mask = jnp.repeat(pair_live[0].astype(jnp.float32), device_pts)
    return (chi * column_mask[None, None, :])[:, :, None, :]


def solution(mesh):
    return jax.shard_map(
        functools.partial(on_device, mesh),
        mesh=mesh,
        in_specs=(P(AXES, None), P(AXES, None), P(), P(), P(), P(), P(), P("pts", None)),
        out_specs=P(None, "pts", "tau", None),
        check_vma=False,
    )
```

```python
import functools

import jax
import jax.numpy as jnp
from jax import lax
from jax.experimental import pallas as pl
from jax.experimental.pallas import tpu as pltpu
from jax.sharding import PartitionSpec as P


AXES = ("pts", "tau")
DIRECT = 4
VMEM = pl.BlockSpec(memory_space=pltpu.VMEM)
PARAMS = pltpu.CompilerParams(vmem_limit_bytes=8 * 1024 * 1024)
SMEM = pl.BlockSpec(memory_space=pltpu.SMEM)


def layout(mesh):
    points, groups = mesh.shape["pts"], mesh.shape["tau"]
    cores = 2 if points % 2 == 0 else 1
    pairs = 2 if points % (2 * cores) == 0 else 1
    return points // (pairs * cores), pairs, cores, groups


def strides_of(mesh):
    sizes = layout(mesh)
    return (sizes[1] * sizes[2] * sizes[3], sizes[2] * sizes[3], sizes[3], 1)


def coordinates(mesh):
    me = lax.axis_index("pts") * mesh.shape["tau"] + lax.axis_index("tau")
    return [lax.rem(lax.div(me, stride), size) for size, stride in zip(layout(mesh), strides_of(mesh))]


def direct(mesh, dim):
    size = layout(mesh)[dim]
    return size <= DIRECT and size & (size - 1) == 0


def gather(mesh, dim, block):
    sizes, stride = layout(mesh), strides_of(mesh)[dim]
    size, n = sizes[dim], sizes[0] * strides_of(mesh)[0]
    if direct(mesh, dim):
        blocks = [block]
        for step in range(size - 1, 0, -1):
            moved = [(i, i + ((((i // stride) % size) ^ step) - (i // stride) % size) * stride) for i in range(n)]
            blocks.append(lax.ppermute(block, AXES, moved))
        return blocks
    mine = coordinates(mesh)[dim]
    firsts = [i for i in range(n) if (i // stride) % size == 0]
    members = [[i + k * stride for k in range(size)] for i in firsts]
    every = lax.all_gather(block, AXES, axis=0, axis_index_groups=members)
    return [every[(mine + k) % size] for k in range(size)]


def halves(x):
    high = x.astype(jnp.bfloat16)
    return high, (x - high.astype(jnp.float32)).astype(jnp.bfloat16)


def dot(a, b):
    return lax.dot_general(a, b, (((1,), (1,)), ((), ())), preferred_element_type=jnp.float32)


def products(left, right):
    (a, a_low), (b, b_low) = halves(left), halves(right)
    return dot(a, b) + (dot(a, b_low) + dot(a_low, b))


def prepare_kernel(tau, weight, frequency, occupied_energy, virtual_energy, live, decay, mixing, mask):
    n_occupied = occupied_energy.shape[1]
    for t in range(tau.shape[0]):
        decay[t : t + 1, :n_occupied] = jnp.exp(occupied_energy[...] * tau[t])
        decay[t : t + 1, n_occupied:] = jnp.exp(-virtual_energy[...] * tau[t])
        for k in range(frequency.shape[0]):
            row = k * tau.shape[0] + t
            angle = jnp.full((1, 128), frequency[k] * tau[t], jnp.float32)
            mixing[row : row + 1, :] = -2.0 * weight[t] * jnp.cos(angle)
    width, blocks = mask.shape[1], live.shape[1]
    column = lax.broadcasted_iota(jnp.int32, (blocks, width), 1)
    block = lax.broadcasted_iota(jnp.int32, (blocks, width), 0)
    spread = jnp.where(lax.div(column, width // blocks) == block, 1.0, 0.0)
    marks = jnp.broadcast_to(live[...].astype(jnp.float32), (8, blocks))
    mask[...] = jnp.dot(marks, spread, preferred_element_type=jnp.float32)


def chi_parts(n_occupied, rows, columns, decay, mixing, n_frequencies):
    n_times = decay.shape[0]
    cols = jnp.concatenate([c[...] for c in columns], axis=0)
    green = []
    for part in (slice(None, n_occupied), slice(n_occupied, None)):
        left = jnp.concatenate([rows[:, part] * decay[t : t + 1, part] for t in range(n_times)], axis=0)
        green.append(products(left, cols[:, part]))
    n_rows = rows.shape[0]
    pair = green[0] * green[1]
    out = []
    for k in range(n_frequencies):
        total = None
        for t in range(n_times):
            row = k * n_times + t
            term = pair[t * n_rows : (t + 1) * n_rows] * mixing[row : row + 1, :1]
            total = term if total is None else total + term
        out.append(total)
    return out


def there_kernel(n_occupied, n_frequencies, rows, *refs):
    columns, (decay, mixing, out) = refs[:-3], refs[-3:]
    for k, chi in enumerate(chi_parts(n_occupied, rows, columns, decay, mixing, n_frequencies)):
        out[k] = chi


def spread_of(mesh, device_pts, pair, width, here):
    sizes = layout(mesh)
    at = coordinates(mesh)
    row = lax.broadcasted_iota(jnp.int32, (width, here), 0)
    column = lax.broadcasted_iota(jnp.int32, (width, here), 1)
    place = lax.div(column, device_pts)
    core = lax.rem(place, sizes[2])
    at_pair = lax.rem(lax.div(place, sizes[2]), sizes[1])
    far = lax.div(place, sizes[2] * sizes[1])
    if direct(mesh, 0):
        step = far ^ at[0]
        nth = (core ^ at[2]) * sizes[0] + jnp.where(step == 0, 0, sizes[0] - step)
    else:
        nth = (core ^ at[2]) * sizes[0] + lax.rem(far - at[0] + sizes[0], sizes[0])
    source = nth * device_pts + lax.rem(column, device_pts)
    return jnp.where((source == row) & (at_pair == pair), 1.0, 0.0)


def here_kernel(mesh, n_occupied, n_frequencies, device_pts, rows, *refs):
    columns, (decay, mixing, mask, out) = refs[:-4], refs[-4:]
    chi = jnp.concatenate(chi_parts(n_occupied, rows, columns, decay, mixing, n_frequencies), axis=0)
    pair = coordinates(mesh)[1]
    spread = spread_of(mesh, device_pts, pair, chi.shape[1], out.shape[1])
    out[...] = jnp.dot(chi, spread, precision=lax.Precision.HIGHEST, preferred_element_type=jnp.float32) * mask[0:1, :]


def join_kernel(mesh, device_pts, here, mask, *refs):
    back, out = refs[:-1], refs[-1]
    total = here[...]
    pair = coordinates(mesh)[1]
    for step, came in enumerate(back, 1):
        chi = came[...].reshape(-1, came.shape[2])
        spread = spread_of(mesh, device_pts, pair ^ step, chi.shape[1], out.shape[1])
        moved = jnp.dot(chi, spread, precision=lax.Precision.HIGHEST, preferred_element_type=jnp.float32)
        total = total + moved * mask[0:1, :]
    out[...] = total


def on_device(
    mesh,
    occupied_values,
    virtual_values,
    occupied_energy,
    virtual_energy,
    tau_points,
    tau_weights,
    frequencies,
    pair_live,
):
    device_pts, n_occupied = occupied_values.shape
    n_all = n_occupied + virtual_values.shape[1]
    n_times, n_frequencies = tau_points.shape[0], frequencies.shape[0]
    far, pairs, cores, groups = layout(mesh)
    n = far * pairs * cores * groups
    f32 = jnp.float32

    own = jnp.pad(occupied_values, ((0, 0), (0, n_all - n_occupied))) + jnp.pad(virtual_values, ((0, 0), (n_occupied, 0)))
    row_blocks = gather(mesh, 3, own)
    group = coordinates(mesh)[3]
    if groups == 2:
        rows = jnp.where(group == 0, jnp.concatenate(row_blocks, 0), jnp.concatenate(row_blocks[::-1], 0))
    else:
        rows = jnp.roll(jnp.concatenate(row_blocks, 0), group * device_pts, axis=0)
    far_blocks = gather(mesh, 0, own)
    row_sets = gather(mesh, 1, rows)
    column_sets = gather(mesh, 2, jnp.concatenate(far_blocks, axis=0))

    decay, mixing, mask = pl.pallas_call(
        prepare_kernel,
        name="prepare",
        out_shape=[
            jax.ShapeDtypeStruct((n_times, n_all), f32),
            jax.ShapeDtypeStruct((n_times * n_frequencies, 128), f32),
            jax.ShapeDtypeStruct((8, far * pairs * cores * device_pts), f32),
        ],
        in_specs=[SMEM] * 3 + [VMEM] * 3,
        out_specs=[VMEM] * 3,
        compiler_params=PARAMS,
    )(tau_points, tau_weights, frequencies, occupied_energy[None], virtual_energy[None], pair_live)

    n_rows, width = rows.shape[0], far * cores * device_pts
    cost = pl.CostEstimate(flops=6 * n_times * n_rows * width * n_all, bytes_accessed=4 * n_all * (width + n_rows), transcendentals=0)
    back = []
    for step in range(1, pairs):
        there = pl.pallas_call(
            functools.partial(there_kernel, n_occupied, n_frequencies),
            name="there",
            out_shape=jax.ShapeDtypeStruct((n_frequencies, n_rows, width), f32),
            in_specs=[VMEM] * (3 + len(column_sets)),
            out_specs=VMEM,
            cost_estimate=cost,
            compiler_params=PARAMS,
        )(row_sets[step], *column_sets, decay, mixing)
        swap = cores * groups * step
        back.append(lax.ppermute(there, AXES, [(i, i ^ swap) for i in range(n)]))
    here = pl.pallas_call(
        functools.partial(here_kernel, mesh, n_occupied, n_frequencies, device_pts),
        name="here",
        out_shape=jax.ShapeDtypeStruct((n_frequencies * n_rows, mask.shape[1]), f32),
        in_specs=[VMEM] * (4 + len(column_sets)),
        out_specs=VMEM,
        cost_estimate=cost,
        compiler_params=PARAMS,
    )(rows, *column_sets, decay, mixing, mask)
    out = pl.pallas_call(
        functools.partial(join_kernel, mesh, device_pts),
        name="join",
        out_shape=jax.ShapeDtypeStruct((n_frequencies * n_rows, mask.shape[1]), f32),
        in_specs=[VMEM] * (2 + len(back)),
        out_specs=VMEM,
        compiler_params=PARAMS,
    )(here, mask, *back)
    return out.reshape(n_frequencies, n_rows, 1, mask.shape[1])


def solution(mesh):
    return jax.shard_map(
        functools.partial(on_device, mesh),
        mesh=mesh,
        in_specs=(P(AXES, None), P(AXES, None), P(), P(), P(), P(), P(), P("pts", None)),
        out_specs=P(None, "pts", "tau", None),
        check_vma=False,
    )
```

```python
import functools

import jax
import jax.numpy as jnp
from jax import lax
from jax.experimental import pallas as pl
from jax.experimental.pallas import tpu as pltpu
from jax.sharding import PartitionSpec as P


AXES = ("pts", "tau")
DIRECT = 4
VMEM = pl.BlockSpec(memory_space=pltpu.VMEM)
PARAMS = pltpu.CompilerParams(vmem_limit_bytes=8 * 1024 * 1024)
SMEM = pl.BlockSpec(memory_space=pltpu.SMEM)


def layout(mesh):
    points, groups = mesh.shape["pts"], mesh.shape["tau"]
    cores = 2 if points % 2 == 0 else 1
    pairs = 2 if points % (2 * cores) == 0 else 1
    return points // (pairs * cores), pairs, cores, groups


def strides_of(mesh):
    sizes = layout(mesh)
    return (sizes[1] * sizes[2] * sizes[3], sizes[2] * sizes[3], sizes[3], 1)


def coordinates(mesh):
    me = lax.axis_index("pts") * mesh.shape["tau"] + lax.axis_index("tau")
    return [lax.rem(lax.div(me, stride), size) for size, stride in zip(layout(mesh), strides_of(mesh))]


def direct(mesh, dim):
    size = layout(mesh)[dim]
    return size <= DIRECT and size & (size - 1) == 0


def crossing(mesh, dim, step):
    return (dim, step) in CROSSING and layout(mesh)[2] == 2 and direct(mesh, dim)


def moves(mesh, dim, step):
    sizes, stride = layout(mesh), strides_of(mesh)[dim]
    pairs = []
    for i in range(sizes[0] * strides_of(mesh)[0]):
        at = (i // stride) % sizes[dim]
        to = i + ((at ^ step) - at) * stride
        if crossing(mesh, dim, step):
            to += (1 - 2 * ((to // sizes[3]) % 2)) * sizes[3]
        pairs.append((i, to))
    return pairs


def gather(mesh, dim, block):
    sizes, stride = layout(mesh), strides_of(mesh)[dim]
    size, n = sizes[dim], sizes[0] * strides_of(mesh)[0]
    if direct(mesh, dim):
        blocks = [block]
        for step in range(size - 1, 0, -1):
            blocks.append(lax.ppermute(block, AXES, moves(mesh, dim, step)))
        return blocks
    mine = coordinates(mesh)[dim]
    firsts = [i for i in range(n) if (i // stride) % size == 0]
    members = [[i + k * stride for k in range(size)] for i in firsts]
    every = lax.all_gather(block, AXES, axis=0, axis_index_groups=members)
    return [every[(mine + k) % size] for k in range(size)]


def halves(x):
    high = x.astype(jnp.bfloat16)
    return high, (x - high.astype(jnp.float32)).astype(jnp.bfloat16)


def dot(a, b):
    return lax.dot_general(a, b, (((1,), (1,)), ((), ())), preferred_element_type=jnp.float32)


def products(left, right):
    (a, a_low), (b, b_low) = halves(left), halves(right)
    return dot(a, b) + (dot(a, b_low) + dot(a_low, b))


def prepare_kernel(tau, weight, frequency, occupied_energy, virtual_energy, live, decay, mixing, mask):
    n_occupied = occupied_energy.shape[1]
    for t in range(tau.shape[0]):
        decay[t : t + 1, :n_occupied] = jnp.exp(occupied_energy[...] * tau[t])
        decay[t : t + 1, n_occupied:] = jnp.exp(-virtual_energy[...] * tau[t])
        for k in range(frequency.shape[0]):
            row = k * tau.shape[0] + t
            angle = jnp.full((1, 128), frequency[k] * tau[t], jnp.float32)
            mixing[row : row + 1, :] = -2.0 * weight[t] * jnp.cos(angle)
    width, blocks = mask.shape[1], live.shape[1]
    column = lax.broadcasted_iota(jnp.int32, (blocks, width), 1)
    block = lax.broadcasted_iota(jnp.int32, (blocks, width), 0)
    spread = jnp.where(lax.div(column, width // blocks) == block, 1.0, 0.0)
    marks = jnp.broadcast_to(live[...].astype(jnp.float32), (8, blocks))
    mask[...] = jnp.dot(marks, spread, preferred_element_type=jnp.float32)


def chi_parts(n_occupied, rows, columns, decay, mixing, n_frequencies):
    n_times = decay.shape[0]
    cols = jnp.concatenate([c[...] for c in columns], axis=0)
    green = []
    for part in (slice(None, n_occupied), slice(n_occupied, None)):
        left = jnp.concatenate([rows[:, part] * decay[t : t + 1, part] for t in range(n_times)], axis=0)
        green.append(products(left, cols[:, part]))
    n_rows = rows.shape[0]
    pair = green[0] * green[1]
    out = []
    for k in range(n_frequencies):
        total = None
        for t in range(n_times):
            row = k * n_times + t
            term = pair[t * n_rows : (t + 1) * n_rows] * mixing[row : row + 1, :1]
            total = term if total is None else total + term
        out.append(total)
    return out


def there_kernel(n_occupied, n_frequencies, rows, *refs):
    columns, (decay, mixing, out) = refs[:-3], refs[-3:]
    for k, chi in enumerate(chi_parts(n_occupied, rows, columns, decay, mixing, n_frequencies)):
        out[k] = chi


def spread_of(mesh, device_pts, pair, core, width, here):
    sizes = layout(mesh)
    far_mine = coordinates(mesh)[0]
    row = lax.broadcasted_iota(jnp.int32, (width, here), 0)
    column = lax.broadcasted_iota(jnp.int32, (width, here), 1)
    place = lax.div(column, device_pts)
    other = lax.rem(place, sizes[2]) ^ core
    at_pair = lax.rem(lax.div(place, sizes[2]), sizes[1])
    far = lax.div(place, sizes[2] * sizes[1])
    if direct(mesh, 0):
        step = far ^ far_mine
        nth = jnp.where(step == 0, 0, sizes[0] - step)
        for k in range(1, sizes[0]):
            if crossing(mesh, 0, k):
                other = jnp.where(step == k, 1 - other, other)
    else:
        nth = lax.rem(far - far_mine + sizes[0], sizes[0])
    source = (other * sizes[0] + nth) * device_pts + lax.rem(column, device_pts)
    return jnp.where((source == row) & (at_pair == pair), 1.0, 0.0)


def here_kernel(mesh, n_occupied, n_frequencies, device_pts, rows, *refs):
    columns, (decay, mixing, mask, out) = refs[:-4], refs[-4:]
    chi = jnp.concatenate(chi_parts(n_occupied, rows, columns, decay, mixing, n_frequencies), axis=0)
    _, pair, core, _ = coordinates(mesh)
    spread = spread_of(mesh, device_pts, pair, core, chi.shape[1], out.shape[1])
    out[...] = jnp.dot(chi, spread, precision=lax.Precision.HIGHEST, preferred_element_type=jnp.float32) * mask[0:1, :]


def join_kernel(mesh, device_pts, here, mask, *refs):
    back, out = refs[:-1], refs[-1]
    total = here[...]
    _, pair, core, _ = coordinates(mesh)
    for step, came in enumerate(back, 1):
        chi = came[...].reshape(-1, came.shape[2])
        spread = spread_of(mesh, device_pts, pair ^ step, 1 - core if crossing(mesh, 1, step) else core, chi.shape[1], out.shape[1])
        moved = jnp.dot(chi, spread, precision=lax.Precision.HIGHEST, preferred_element_type=jnp.float32)
        total = total + moved * mask[0:1, :]
    out[...] = total


def on_device(
    mesh,
    occupied_values,
    virtual_values,
    occupied_energy,
    virtual_energy,
    tau_points,
    tau_weights,
    frequencies,
    pair_live,
):
    device_pts, n_occupied = occupied_values.shape
    n_all = n_occupied + virtual_values.shape[1]
    n_times, n_frequencies = tau_points.shape[0], frequencies.shape[0]
    far, pairs, cores, groups = layout(mesh)
    f32 = jnp.float32

    own = jnp.pad(occupied_values, ((0, 0), (0, n_all - n_occupied))) + jnp.pad(virtual_values, ((0, 0), (n_occupied, 0)))
    row_blocks = gather(mesh, 3, own)
    group = coordinates(mesh)[3]
    if groups == 2:
        rows = jnp.where(group == 0, jnp.concatenate(row_blocks, 0), jnp.concatenate(row_blocks[::-1], 0))
    else:
        rows = jnp.roll(jnp.concatenate(row_blocks, 0), group * device_pts, axis=0)
    far_blocks = gather(mesh, 0, own)
    row_sets = gather(mesh, 1, rows)
    pieces = [jnp.concatenate(far_blocks, axis=0)]
    column_sets = []
    for piece in pieces:
        column_sets += gather(mesh, 2, piece)

    decay, mixing, mask = pl.pallas_call(
        prepare_kernel,
        name="prepare",
        out_shape=[
            jax.ShapeDtypeStruct((n_times, n_all), f32),
            jax.ShapeDtypeStruct((n_times * n_frequencies, 128), f32),
            jax.ShapeDtypeStruct((8, far * pairs * cores * device_pts), f32),
        ],
        in_specs=[SMEM] * 3 + [VMEM] * 3,
        out_specs=[VMEM] * 3,
        compiler_params=PARAMS,
    )(tau_points, tau_weights, frequencies, occupied_energy[None], virtual_energy[None], pair_live)

    n_rows, width = rows.shape[0], far * cores * device_pts
    cost = pl.CostEstimate(flops=6 * n_times * n_rows * width * n_all, bytes_accessed=4 * n_all * (width + n_rows), transcendentals=0)
    back = []
    for step in range(1, pairs):
        there = pl.pallas_call(
            functools.partial(there_kernel, n_occupied, n_frequencies),
            name="there",
            out_shape=jax.ShapeDtypeStruct((n_frequencies, n_rows, width), f32),
            in_specs=[VMEM] * (3 + len(column_sets)),
            out_specs=VMEM,
            cost_estimate=cost,
            compiler_params=PARAMS,
        )(row_sets[step], *column_sets, decay, mixing)
        back.append(lax.ppermute(there, AXES, moves(mesh, 1, step)))
    here = pl.pallas_call(
        functools.partial(here_kernel, mesh, n_occupied, n_frequencies, device_pts),
        name="here",
        out_shape=jax.ShapeDtypeStruct((n_frequencies * n_rows, mask.shape[1]), f32),
        in_specs=[VMEM] * (4 + len(column_sets)),
        out_specs=VMEM,
        cost_estimate=cost,
        compiler_params=PARAMS,
    )(rows, *column_sets, decay, mixing, mask)
    out = pl.pallas_call(
        functools.partial(join_kernel, mesh, device_pts),
        name="join",
        out_shape=jax.ShapeDtypeStruct((n_frequencies * n_rows, mask.shape[1]), f32),
        in_specs=[VMEM] * (2 + len(back)),
        out_specs=VMEM,
        compiler_params=PARAMS,
    )(here, mask, *back)
    return out.reshape(n_frequencies, n_rows, 1, mask.shape[1])


CROSSING = ((0, 1), (1, 1))


def solution(mesh):
    return jax.shard_map(
        functools.partial(on_device, mesh),
        mesh=mesh,
        in_specs=(P(AXES, None), P(AXES, None), P(), P(), P(), P(), P(), P("pts", None)),
        out_specs=P(None, "pts", "tau", None),
        check_vma=False,
    )
```

```python
import functools

import jax
import jax.numpy as jnp
from jax import lax
from jax.experimental import pallas as pl
from jax.experimental.pallas import tpu as pltpu
from jax.sharding import PartitionSpec as P


AXES = ("pts", "tau")
CROSSING = ((1, 1),)
VMEM = pl.BlockSpec(memory_space=pltpu.VMEM)
PARAMS = pltpu.CompilerParams(vmem_limit_bytes=8 * 1024 * 1024)
SMEM = pl.BlockSpec(memory_space=pltpu.SMEM)


def layout(mesh):
    points, groups = mesh.shape["pts"], mesh.shape["tau"]
    cores = 2 if points % 2 == 0 else 1
    pairs = 2 if points % (2 * cores) == 0 else 1
    return points // (pairs * cores), pairs, cores, groups


def strides_of(mesh):
    sizes = layout(mesh)
    return (sizes[1] * sizes[2] * sizes[3], sizes[2] * sizes[3], sizes[3], 1)


def coordinates(mesh):
    me = lax.axis_index("pts") * mesh.shape["tau"] + lax.axis_index("tau")
    return [lax.rem(lax.div(me, stride), size) for size, stride in zip(layout(mesh), strides_of(mesh))]


def direct(mesh, dim):
    size = layout(mesh)[dim]
    return size in (1, 2, 4) and (dim != 3 or size < 4)


def crossing(mesh, dim, step):
    return (dim, step) in CROSSING and layout(mesh)[2] == 2 and direct(mesh, dim)


def ring(at):
    return at ^ (at >> 1)


def moves(mesh, dim, step):
    sizes, stride = layout(mesh), strides_of(mesh)[dim]
    pairs = []
    for i in range(sizes[0] * strides_of(mesh)[0]):
        at = (i // stride) % sizes[dim]
        to = i + (ring((ring(at) + step) % sizes[dim]) - at) * stride
        if crossing(mesh, dim, step):
            to += (1 - 2 * ((to // sizes[3]) % 2)) * sizes[3]
        pairs.append((i, to))
    return pairs


def gather(mesh, dim, block):
    sizes, stride = layout(mesh), strides_of(mesh)[dim]
    size, n = sizes[dim], sizes[0] * strides_of(mesh)[0]
    if direct(mesh, dim):
        blocks = [block]
        for step in range(size - 1, 0, -1):
            blocks.append(lax.ppermute(block, AXES, moves(mesh, dim, step)))
        return blocks
    mine = coordinates(mesh)[dim]
    firsts = [i for i in range(n) if (i // stride) % size == 0]
    members = [[i + k * stride for k in range(size)] for i in firsts]
    every = lax.all_gather(block, AXES, axis=0, axis_index_groups=members)
    return [every[(mine + k) % size] for k in range(size)]


def halves(x):
    high = x.astype(jnp.bfloat16)
    return high, (x - high.astype(jnp.float32)).astype(jnp.bfloat16)


def dot(a, b):
    return lax.dot_general(a, b, (((1,), (1,)), ((), ())), preferred_element_type=jnp.float32)


def products(left, right):
    (a, a_low), (b, b_low) = halves(left), halves(right)
    return dot(a, b) + (dot(a, b_low) + dot(a_low, b))


def prepare_kernel(tau, weight, frequency, occupied_energy, virtual_energy, live, decay, mixing, mask):
    n_occupied = occupied_energy.shape[1]
    for t in range(tau.shape[0]):
        decay[t : t + 1, :n_occupied] = jnp.exp(occupied_energy[...] * tau[t])
        decay[t : t + 1, n_occupied:] = jnp.exp(-virtual_energy[...] * tau[t])
        for k in range(frequency.shape[0]):
            row = k * tau.shape[0] + t
            angle = jnp.full((1, 128), frequency[k] * tau[t], jnp.float32)
            mixing[row : row + 1, :] = -2.0 * weight[t] * jnp.cos(angle)
    width, blocks = mask.shape[1], live.shape[1]
    column = lax.broadcasted_iota(jnp.int32, (blocks, width), 1)
    block = lax.broadcasted_iota(jnp.int32, (blocks, width), 0)
    spread = jnp.where(lax.div(column, width // blocks) == block, 1.0, 0.0)
    marks = jnp.broadcast_to(live[...].astype(jnp.float32), (8, blocks))
    mask[...] = jnp.dot(marks, spread, preferred_element_type=jnp.float32)


def chi_parts(n_occupied, rows, columns, decay, mixing, n_frequencies):
    n_times = decay.shape[0]
    cols = jnp.concatenate([c[...] for c in columns], axis=0)
    green = []
    for part in (slice(None, n_occupied), slice(n_occupied, None)):
        left = jnp.concatenate([rows[:, part] * decay[t : t + 1, part] for t in range(n_times)], axis=0)
        green.append(products(left, cols[:, part]))
    n_rows = rows.shape[0]
    pair = green[0] * green[1]
    out = []
    for k in range(n_frequencies):
        total = None
        for t in range(n_times):
            row = k * n_times + t
            term = pair[t * n_rows : (t + 1) * n_rows] * mixing[row : row + 1, :1]
            total = term if total is None else total + term
        out.append(total)
    return out


def there_kernel(n_occupied, n_frequencies, rows, *refs):
    columns, (decay, mixing, out) = refs[:-3], refs[-3:]
    for k, chi in enumerate(chi_parts(n_occupied, rows, columns, decay, mixing, n_frequencies)):
        out[k] = chi


def spread_of(mesh, device_pts, pair, core, width, here):
    sizes = layout(mesh)
    far_mine = coordinates(mesh)[0]
    row = lax.broadcasted_iota(jnp.int32, (width, here), 0)
    column = lax.broadcasted_iota(jnp.int32, (width, here), 1)
    place = lax.div(column, device_pts)
    other = lax.rem(place, sizes[2]) ^ core
    at_pair = lax.rem(lax.div(place, sizes[2]), sizes[1])
    far = lax.div(place, sizes[2] * sizes[1])
    if direct(mesh, 0):
        step = (ring(far_mine) - ring(far)) & (sizes[0] - 1)
        nth = jnp.where(step == 0, 0, sizes[0] - step)
        for k in range(1, sizes[0]):
            if crossing(mesh, 0, k):
                other = jnp.where(step == k, 1 - other, other)
    else:
        nth = lax.rem(far - far_mine + sizes[0], sizes[0])
    source = (other * sizes[0] + nth) * device_pts + lax.rem(column, device_pts)
    return jnp.where((source == row) & (at_pair == pair), 1.0, 0.0)


def here_kernel(mesh, n_occupied, n_frequencies, device_pts, rows, *refs):
    columns, (decay, mixing, mask, out) = refs[:-4], refs[-4:]
    chi = jnp.concatenate(chi_parts(n_occupied, rows, columns, decay, mixing, n_frequencies), axis=0)
    _, pair, core, _ = coordinates(mesh)
    spread = spread_of(mesh, device_pts, pair, core, chi.shape[1], out.shape[1])
    out[...] = jnp.dot(chi, spread, precision=lax.Precision.HIGHEST, preferred_element_type=jnp.float32) * mask[0:1, :]


def join_kernel(mesh, device_pts, here, mask, *refs):
    back, out = refs[:-1], refs[-1]
    total = here[...]
    _, pair, core, _ = coordinates(mesh)
    for step, came in enumerate(back, 1):
        chi = came[...].reshape(-1, came.shape[2])
        spread = spread_of(mesh, device_pts, pair ^ step, 1 - core if crossing(mesh, 1, step) else core, chi.shape[1], out.shape[1])
        moved = jnp.dot(chi, spread, precision=lax.Precision.HIGHEST, preferred_element_type=jnp.float32)
        total = total + moved * mask[0:1, :]
    out[...] = total


def on_device(
    mesh,
    occupied_values,
    virtual_values,
    occupied_energy,
    virtual_energy,
    tau_points,
    tau_weights,
    frequencies,
    pair_live,
):
    device_pts, n_occupied = occupied_values.shape
    n_all = n_occupied + virtual_values.shape[1]
    n_times, n_frequencies = tau_points.shape[0], frequencies.shape[0]
    far, pairs, cores, groups = layout(mesh)
    f32 = jnp.float32

    own = jnp.pad(occupied_values, ((0, 0), (0, n_all - n_occupied))) + jnp.pad(virtual_values, ((0, 0), (n_occupied, 0)))
    row_blocks = gather(mesh, 3, own)
    group = coordinates(mesh)[3]
    if groups == 2:
        rows = jnp.where(group == 0, jnp.concatenate(row_blocks, 0), jnp.concatenate(row_blocks[::-1], 0))
    else:
        rows = jnp.roll(jnp.concatenate(row_blocks, 0), group * device_pts, axis=0)
    far_blocks = gather(mesh, 0, own)
    row_sets = gather(mesh, 1, rows)
    column_sets = gather(mesh, 2, jnp.concatenate(far_blocks, axis=0))

    decay, mixing, mask = pl.pallas_call(
        prepare_kernel,
        name="prepare",
        out_shape=[
            jax.ShapeDtypeStruct((n_times, n_all), f32),
            jax.ShapeDtypeStruct((n_times * n_frequencies, 128), f32),
            jax.ShapeDtypeStruct((8, far * pairs * cores * device_pts), f32),
        ],
        in_specs=[SMEM] * 3 + [VMEM] * 3,
        out_specs=[VMEM] * 3,
        compiler_params=PARAMS,
    )(tau_points, tau_weights, frequencies, occupied_energy[None], virtual_energy[None], pair_live)

    n_rows, width = rows.shape[0], far * cores * device_pts
    cost = pl.CostEstimate(flops=6 * n_times * n_rows * width * n_all, bytes_accessed=4 * n_all * (width + n_rows), transcendentals=0)
    back = []
    for step in range(1, pairs):
        there = pl.pallas_call(
            functools.partial(there_kernel, n_occupied, n_frequencies),
            name="there",
            out_shape=jax.ShapeDtypeStruct((n_frequencies, n_rows, width), f32),
            in_specs=[VMEM] * (3 + len(column_sets)),
            out_specs=VMEM,
            cost_estimate=cost,
            compiler_params=PARAMS,
        )(row_sets[step], *column_sets, decay, mixing)
        back.append(lax.ppermute(there, AXES, moves(mesh, 1, step)))
    here = pl.pallas_call(
        functools.partial(here_kernel, mesh, n_occupied, n_frequencies, device_pts),
        name="here",
        out_shape=jax.ShapeDtypeStruct((n_frequencies * n_rows, mask.shape[1]), f32),
        in_specs=[VMEM] * (4 + len(column_sets)),
        out_specs=VMEM,
        cost_estimate=cost,
        compiler_params=PARAMS,
    )(rows, *column_sets, decay, mixing, mask)
    out = pl.pallas_call(
        functools.partial(join_kernel, mesh, device_pts),
        name="join",
        out_shape=jax.ShapeDtypeStruct((n_frequencies * n_rows, mask.shape[1]), f32),
        in_specs=[VMEM] * (2 + len(back)),
        out_specs=VMEM,
        compiler_params=PARAMS,
    )(here, mask, *back)
    return out.reshape(n_frequencies, n_rows, 1, mask.shape[1])


def solution(mesh):
    return jax.shard_map(
        functools.partial(on_device, mesh),
        mesh=mesh,
        in_specs=(P(AXES, None), P(AXES, None), P(), P(), P(), P(), P(), P("pts", None)),
        out_specs=P(None, "pts", "tau", None),
        check_vma=False,
    )
```

```python
import functools

import jax
import jax.numpy as jnp
from jax import lax
from jax.experimental import pallas as pl
from jax.experimental.pallas import tpu as pltpu
from jax.sharding import PartitionSpec as P


AXES = ("pts", "tau")
CROSSING = ((1, 1),)
VMEM = pl.BlockSpec(memory_space=pltpu.VMEM)
PARAMS = pltpu.CompilerParams(vmem_limit_bytes=8 * 1024 * 1024)
SMEM = pl.BlockSpec(memory_space=pltpu.SMEM)


def layout(mesh):
    points, groups = mesh.shape["pts"], mesh.shape["tau"]
    cores = 2 if points % 2 == 0 else 1
    pairs = 2 if points % (2 * cores) == 0 else 1
    return points // (pairs * cores), pairs, cores, groups


def strides_of(mesh):
    sizes = layout(mesh)
    return (sizes[1] * sizes[2] * sizes[3], sizes[2] * sizes[3], sizes[3], 1)


def coordinates(mesh):
    me = lax.axis_index("pts") * mesh.shape["tau"] + lax.axis_index("tau")
    return [lax.rem(lax.div(me, stride), size) for size, stride in zip(layout(mesh), strides_of(mesh))]


def direct(mesh, dim):
    size = layout(mesh)[dim]
    return size in (1, 2, 4) and (dim != 3 or size < 4)


def crossing(mesh, dim, step):
    return (dim, step) in CROSSING and layout(mesh)[2] == 2 and direct(mesh, dim)


def ring(at):
    return at ^ (at >> 1)


def moves(mesh, dim, step):
    sizes, stride = layout(mesh), strides_of(mesh)[dim]
    pairs = []
    for i in range(sizes[0] * strides_of(mesh)[0]):
        at = (i // stride) % sizes[dim]
        to = i + (ring((ring(at) + step) % sizes[dim]) - at) * stride
        if crossing(mesh, dim, step):
            to += (1 - 2 * ((to // sizes[3]) % 2)) * sizes[3]
        pairs.append((i, to))
    return pairs


def gather(mesh, dim, block):
    sizes, stride = layout(mesh), strides_of(mesh)[dim]
    size, n = sizes[dim], sizes[0] * strides_of(mesh)[0]
    if direct(mesh, dim):
        blocks = [block]
        for step in range(size - 1, 0, -1):
            blocks.append(lax.ppermute(block, AXES, moves(mesh, dim, step)))
        return blocks
    mine = coordinates(mesh)[dim]
    firsts = [i for i in range(n) if (i // stride) % size == 0]
    members = [[i + k * stride for k in range(size)] for i in firsts]
    every = lax.all_gather(block, AXES, axis=0, axis_index_groups=members)
    return [every[(mine + k) % size] for k in range(size)]


def halves(x):
    high = x.astype(jnp.bfloat16)
    return high, (x - high.astype(jnp.float32)).astype(jnp.bfloat16)


def dot(a, b):
    return lax.dot_general(a, b, (((1,), (1,)), ((), ())), preferred_element_type=jnp.float32)


def products(left, right):
    (a, a_low), (b, b_low) = halves(left), halves(right)
    return dot(a, b) + (dot(a, b_low) + dot(a_low, b))


def prepare_kernel(mesh, device_pts, tau, weight, frequency, occupied_energy, virtual_energy, live, decay, mixing, mask, spread):
    n_occupied = occupied_energy.shape[1]
    for t in range(tau.shape[0]):
        decay[t : t + 1, :n_occupied] = jnp.exp(occupied_energy[...] * tau[t])
        decay[t : t + 1, n_occupied:] = jnp.exp(-virtual_energy[...] * tau[t])
        for k in range(frequency.shape[0]):
            row = k * tau.shape[0] + t
            angle = jnp.full((1, 128), frequency[k] * tau[t], jnp.float32)
            mixing[row : row + 1, :] = -2.0 * weight[t] * jnp.cos(angle)
    width, blocks = mask.shape[1], live.shape[1]
    column = lax.broadcasted_iota(jnp.int32, (blocks, width), 1)
    block = lax.broadcasted_iota(jnp.int32, (blocks, width), 0)
    repeat = jnp.where(lax.div(column, width // blocks) == block, 1.0, 0.0)
    marks = jnp.broadcast_to(live[...].astype(jnp.float32), (8, blocks))
    mask[...] = jnp.dot(marks, repeat, preferred_element_type=jnp.float32)
    _, pair, core, _ = coordinates(mesh)
    spread[...] = spread_of(mesh, device_pts, pair, core, spread.shape[0], width).astype(jnp.bfloat16)


def chi_parts(n_occupied, rows, columns, decay, mixing, n_frequencies):
    n_times = decay.shape[0]
    cols = jnp.concatenate([c[...] for c in columns], axis=0)
    green = []
    for part in (slice(None, n_occupied), slice(n_occupied, None)):
        left = jnp.concatenate([rows[:, part] * decay[t : t + 1, part] for t in range(n_times)], axis=0)
        green.append(products(left, cols[:, part]))
    n_rows = rows.shape[0]
    pair = green[0] * green[1]
    out = []
    for k in range(n_frequencies):
        total = None
        for t in range(n_times):
            row = k * n_times + t
            term = pair[t * n_rows : (t + 1) * n_rows] * mixing[row : row + 1, :1]
            total = term if total is None else total + term
        out.append(total)
    return out


def spread_of(mesh, device_pts, pair, core, width, here):
    sizes = layout(mesh)
    far_mine = coordinates(mesh)[0]
    row = lax.broadcasted_iota(jnp.int32, (width, here), 0)
    column = lax.broadcasted_iota(jnp.int32, (width, here), 1)
    place = lax.div(column, device_pts)
    other = lax.rem(place, sizes[2]) ^ core
    at_pair = lax.rem(lax.div(place, sizes[2]), sizes[1])
    far = lax.div(place, sizes[2] * sizes[1])
    if direct(mesh, 0):
        step = (ring(far_mine) - ring(far)) & (sizes[0] - 1)
        nth = jnp.where(step == 0, 0, sizes[0] - step)
        for k in range(1, sizes[0]):
            if crossing(mesh, 0, k):
                other = jnp.where(step == k, 1 - other, other)
    else:
        nth = lax.rem(far - far_mine + sizes[0], sizes[0])
    source = (other * sizes[0] + nth) * device_pts + lax.rem(column, device_pts)
    return jnp.where((source == row) & (at_pair == pair), 1.0, 0.0)


def chi_kernel(n_occupied, n_frequencies, rows, *refs):
    columns, (decay, mixing, spread, out) = refs[:-4], refs[-4:]
    chi = jnp.concatenate(chi_parts(n_occupied, rows, columns, decay, mixing, n_frequencies), axis=0)
    total = None
    for _ in range(3):
        part = chi.astype(jnp.bfloat16)
        chi = chi - part.astype(jnp.float32)
        moved = jnp.dot(part, spread[...], preferred_element_type=jnp.float32)
        total = moved if total is None else total + moved
    out[...] = total


def on_device(
    mesh,
    occupied_values,
    virtual_values,
    occupied_energy,
    virtual_energy,
    tau_points,
    tau_weights,
    frequencies,
    pair_live,
):
    device_pts, n_occupied = occupied_values.shape
    n_all = n_occupied + virtual_values.shape[1]
    n_times, n_frequencies = tau_points.shape[0], frequencies.shape[0]
    far, pairs, cores, groups = layout(mesh)
    f32 = jnp.float32

    own = jnp.pad(occupied_values, ((0, 0), (0, n_all - n_occupied))) + jnp.pad(virtual_values, ((0, 0), (n_occupied, 0)))
    row_blocks = gather(mesh, 3, own)
    group = coordinates(mesh)[3]
    if groups == 2:
        rows = jnp.where(group == 0, jnp.concatenate(row_blocks, 0), jnp.concatenate(row_blocks[::-1], 0))
    else:
        rows = jnp.roll(jnp.concatenate(row_blocks, 0), group * device_pts, axis=0)
    far_blocks = gather(mesh, 0, own)
    row_sets = gather(mesh, 1, rows)
    column_sets = gather(mesh, 2, jnp.concatenate(far_blocks, axis=0))

    decay, mixing, mask, spread = pl.pallas_call(
        functools.partial(prepare_kernel, mesh, device_pts),
        name="prepare",
        out_shape=[
            jax.ShapeDtypeStruct((n_times, n_all), f32),
            jax.ShapeDtypeStruct((n_times * n_frequencies, 128), f32),
            jax.ShapeDtypeStruct((8, far * pairs * cores * device_pts), f32),
            jax.ShapeDtypeStruct((far * cores * device_pts, far * pairs * cores * device_pts), jnp.bfloat16),
        ],
        in_specs=[SMEM] * 3 + [VMEM] * 3,
        out_specs=[VMEM] * 4,
        compiler_params=PARAMS,
    )(tau_points, tau_weights, frequencies, occupied_energy[None], virtual_energy[None], pair_live)

    n_rows, width = rows.shape[0], far * cores * device_pts
    cost = pl.CostEstimate(flops=6 * n_times * n_rows * width * n_all, bytes_accessed=4 * n_all * (width + n_rows), transcendentals=0)

    def chi_of(part):
        return pl.pallas_call(
            functools.partial(chi_kernel, n_occupied, n_frequencies),
            out_shape=jax.ShapeDtypeStruct((n_frequencies * n_rows, mask.shape[1]), f32),
            in_specs=[VMEM] * (4 + len(column_sets)),
            out_specs=VMEM,
            cost_estimate=cost,
            compiler_params=PARAMS,
        )(part, *column_sets, decay, mixing, spread)

    back = []
    for step in range(1, pairs):
        there = chi_of(row_sets[step])
        back.append(lax.ppermute(there, AXES, moves(mesh, 1, step)))
    out = (chi_of(rows) + sum(back)) * mask[0:1, :]
    return out.reshape(n_frequencies, n_rows, 1, mask.shape[1])


def solution(mesh):
    return jax.shard_map(
        functools.partial(on_device, mesh),
        mesh=mesh,
        in_specs=(P(AXES, None), P(AXES, None), P(), P(), P(), P(), P(), P("pts", None)),
        out_specs=P(None, "pts", "tau", None),
        check_vma=False,
    )
```

```python
import functools

import jax
import jax.numpy as jnp
from jax import lax
from jax.experimental import pallas as pl
from jax.experimental.pallas import tpu as pltpu
from jax.sharding import PartitionSpec as P


AXES = ("pts", "tau")
CROSSING = ((1, 1),)
VMEM = pl.BlockSpec(memory_space=pltpu.VMEM)
PARAMS = pltpu.CompilerParams(vmem_limit_bytes=8 * 1024 * 1024)
SMEM = pl.BlockSpec(memory_space=pltpu.SMEM)


def layout(mesh):
    points, groups = mesh.shape["pts"], mesh.shape["tau"]
    cores = 2 if points % 2 == 0 else 1
    pairs = 2 if points % (2 * cores) == 0 else 1
    return points // (pairs * cores), pairs, cores, groups


def strides_of(mesh):
    sizes = layout(mesh)
    return (sizes[1] * sizes[2] * sizes[3], sizes[2] * sizes[3], sizes[3], 1)


def coordinates(mesh):
    me = lax.axis_index("pts") * mesh.shape["tau"] + lax.axis_index("tau")
    return [lax.rem(lax.div(me, stride), size) for size, stride in zip(layout(mesh), strides_of(mesh))]


def direct(mesh, dim):
    size = layout(mesh)[dim]
    return size in (1, 2, 4) and (dim != 3 or size < 4)


def crossing(mesh, dim, step):
    return (dim, step) in CROSSING and layout(mesh)[2] == 2 and direct(mesh, dim)


def ring(at):
    return at ^ (at >> 1)


def moves(mesh, dim, step):
    sizes, stride = layout(mesh), strides_of(mesh)[dim]
    pairs = []
    for i in range(sizes[0] * strides_of(mesh)[0]):
        at = (i // stride) % sizes[dim]
        to = i + (ring((ring(at) + step) % sizes[dim]) - at) * stride
        if crossing(mesh, dim, step):
            to += (1 - 2 * ((to // sizes[3]) % 2)) * sizes[3]
        pairs.append((i, to))
    return pairs


def gather(mesh, dim, block):
    sizes, stride = layout(mesh), strides_of(mesh)[dim]
    size, n = sizes[dim], sizes[0] * strides_of(mesh)[0]
    if direct(mesh, dim):
        blocks = [block]
        for step in range(size - 1, 0, -1):
            blocks.append(lax.ppermute(block, AXES, moves(mesh, dim, step)))
        return blocks
    mine = coordinates(mesh)[dim]
    firsts = [i for i in range(n) if (i // stride) % size == 0]
    members = [[i + k * stride for k in range(size)] for i in firsts]
    every = lax.all_gather(block, AXES, axis=0, axis_index_groups=members)
    return [every[(mine + k) % size] for k in range(size)]


def halves(x):
    high = x.astype(jnp.bfloat16)
    return high, (x - high.astype(jnp.float32)).astype(jnp.bfloat16)


def dot(a, b):
    return lax.dot_general(a, b, (((1,), (1,)), ((), ())), preferred_element_type=jnp.float32)


def prepare_kernel(mesh, device_pts, tau, weight, frequency, occupied_energy, virtual_energy, live, decay, mixing, mask, spread):
    n_occupied = occupied_energy.shape[1]
    for t in range(tau.shape[0]):
        decay[t : t + 1, :n_occupied] = jnp.exp(occupied_energy[...] * tau[t])
        decay[t : t + 1, n_occupied:] = jnp.exp(-virtual_energy[...] * tau[t])
        for k in range(frequency.shape[0]):
            row = k * tau.shape[0] + t
            angle = jnp.full((1, 128), frequency[k] * tau[t], jnp.float32)
            mixing[row : row + 1, :] = -2.0 * weight[t] * jnp.cos(angle)
    width, blocks = mask.shape[1], live.shape[1]
    column = lax.broadcasted_iota(jnp.int32, (blocks, width), 1)
    block = lax.broadcasted_iota(jnp.int32, (blocks, width), 0)
    repeat = jnp.where(lax.div(column, width // blocks) == block, 1.0, 0.0)
    marks = jnp.broadcast_to(live[...].astype(jnp.float32), (8, blocks))
    mask[...] = jnp.dot(marks, repeat, preferred_element_type=jnp.float32)
    _, pair, core, _ = coordinates(mesh)
    spread[...] = spread_of(mesh, device_pts, pair, core, spread.shape[0], width).astype(jnp.bfloat16)


def scale_kernel(rows, decay, left, left_low):
    left[...], left_low[...] = halves(jnp.concatenate([rows[...] * decay[t : t + 1, :] for t in range(decay.shape[0])], axis=0))


def chi_parts(n_occupied, n_frequencies, left, left_low, columns, mixing):
    cols = jnp.concatenate([c[...] for c in columns], axis=0)
    n_times = mixing.shape[0] // n_frequencies
    green = []
    for part in (slice(None, n_occupied), slice(n_occupied, None)):
        right, right_low = halves(cols[:, part])
        a, a_low = left[:, part], left_low[:, part]
        green.append(dot(a, right) + (dot(a, right_low) + dot(a_low, right)))
    n_rows = left.shape[0] // n_times
    pair = green[0] * green[1]
    out = []
    for k in range(n_frequencies):
        total = None
        for t in range(n_times):
            row = k * n_times + t
            term = pair[t * n_rows : (t + 1) * n_rows] * mixing[row : row + 1, :1]
            total = term if total is None else total + term
        out.append(total)
    return out


def spread_of(mesh, device_pts, pair, core, width, here):
    sizes = layout(mesh)
    far_mine = coordinates(mesh)[0]
    row = lax.broadcasted_iota(jnp.int32, (width, here), 0)
    column = lax.broadcasted_iota(jnp.int32, (width, here), 1)
    place = lax.div(column, device_pts)
    other = lax.rem(place, sizes[2]) ^ core
    at_pair = lax.rem(lax.div(place, sizes[2]), sizes[1])
    far = lax.div(place, sizes[2] * sizes[1])
    if direct(mesh, 0):
        step = (ring(far_mine) - ring(far)) & (sizes[0] - 1)
        nth = jnp.where(step == 0, 0, sizes[0] - step)
        for k in range(1, sizes[0]):
            if crossing(mesh, 0, k):
                other = jnp.where(step == k, 1 - other, other)
    else:
        nth = lax.rem(far - far_mine + sizes[0], sizes[0])
    source = (other * sizes[0] + nth) * device_pts + lax.rem(column, device_pts)
    return jnp.where((source == row) & (at_pair == pair), 1.0, 0.0)


def chi_kernel(n_occupied, n_frequencies, left, left_low, *refs):
    columns, (mixing, spread, out) = refs[:-3], refs[-3:]
    chi = jnp.concatenate(chi_parts(n_occupied, n_frequencies, left, left_low, columns, mixing), axis=0)
    total = None
    for _ in range(3):
        part = chi.astype(jnp.bfloat16)
        chi = chi - part.astype(jnp.float32)
        moved = jnp.dot(part, spread[...], preferred_element_type=jnp.float32)
        total = moved if total is None else total + moved
    out[...] = total


def on_device(
    mesh,
    occupied_values,
    virtual_values,
    occupied_energy,
    virtual_energy,
    tau_points,
    tau_weights,
    frequencies,
    pair_live,
):
    device_pts, n_occupied = occupied_values.shape
    n_all = n_occupied + virtual_values.shape[1]
    n_times, n_frequencies = tau_points.shape[0], frequencies.shape[0]
    far, pairs, cores, groups = layout(mesh)
    f32 = jnp.float32

    own = jnp.pad(occupied_values, ((0, 0), (0, n_all - n_occupied))) + jnp.pad(virtual_values, ((0, 0), (n_occupied, 0)))
    row_blocks = gather(mesh, 3, own)
    group = coordinates(mesh)[3]
    if groups == 2:
        rows = jnp.where(group == 0, jnp.concatenate(row_blocks, 0), jnp.concatenate(row_blocks[::-1], 0))
    else:
        rows = jnp.roll(jnp.concatenate(row_blocks, 0), group * device_pts, axis=0)
    far_blocks = gather(mesh, 0, own)
    row_sets = gather(mesh, 1, rows)
    column_sets = gather(mesh, 2, jnp.concatenate(far_blocks, axis=0))

    decay, mixing, mask, spread = pl.pallas_call(
        functools.partial(prepare_kernel, mesh, device_pts),
        name="prepare",
        out_shape=[
            jax.ShapeDtypeStruct((n_times, n_all), f32),
            jax.ShapeDtypeStruct((n_times * n_frequencies, 128), f32),
            jax.ShapeDtypeStruct((8, far * pairs * cores * device_pts), f32),
            jax.ShapeDtypeStruct((far * cores * device_pts, far * pairs * cores * device_pts), jnp.bfloat16),
        ],
        in_specs=[SMEM] * 3 + [VMEM] * 3,
        out_specs=[VMEM] * 4,
        compiler_params=PARAMS,
    )(tau_points, tau_weights, frequencies, occupied_energy[None], virtual_energy[None], pair_live)

    n_rows, width = rows.shape[0], far * cores * device_pts
    cost = pl.CostEstimate(flops=6 * n_times * n_rows * width * n_all, bytes_accessed=4 * n_all * (width + n_rows), transcendentals=0)

    def chi_of(part):
        half = jax.ShapeDtypeStruct((n_times * n_rows, n_all), jnp.bfloat16)
        left, left_low = pl.pallas_call(
            scale_kernel,
            name="scale",
            out_shape=[half, half],
            in_specs=[VMEM] * 2,
            out_specs=[VMEM] * 2,
            compiler_params=PARAMS,
        )(part, decay)
        return pl.pallas_call(
            functools.partial(chi_kernel, n_occupied, n_frequencies),
            out_shape=jax.ShapeDtypeStruct((n_frequencies * n_rows, mask.shape[1]), f32),
            in_specs=[VMEM] * (4 + len(column_sets)),
            out_specs=VMEM,
            cost_estimate=cost,
            compiler_params=PARAMS,
        )(left, left_low, *column_sets, mixing, spread)

    back = []
    for step in range(1, pairs):
        there = chi_of(row_sets[step])
        back.append(lax.ppermute(there, AXES, moves(mesh, 1, step)))
    out = (chi_of(rows) + sum(back)) * mask[0:1, :]
    return out.reshape(n_frequencies, n_rows, 1, mask.shape[1])


def solution(mesh):
    return jax.shard_map(
        functools.partial(on_device, mesh),
        mesh=mesh,
        in_specs=(P(AXES, None), P(AXES, None), P(), P(), P(), P(), P(), P("pts", None)),
        out_specs=P(None, "pts", "tau", None),
        check_vma=False,
    )
```
